32 devices in a mesh: groups: 2 (over y), inner: 4 (over z), outer: 2 (over x), head: 2 (over core).
Axes of the slice: x: 2, y: 2, z: 4, core: 2. Of those that a mesh axis runs over, the one named last changes fastest.
Arguments:
- queries: bfloat16 [4, 512, 8, 128], P(('groups', 'outer'), 'inner', 'head'), parts along dimension 0, may hold values from -112 to 112
- keys: bfloat16 [4, 512, 128], P(('groups', 'outer'), 'inner'), parts along dimension 0, may hold values from -4 to 4
- values: bfloat16 [4, 512, 128], P(('groups', 'outer'), 'inner'), parts along dimension 0, may hold values from -6 to 6
- out: bfloat16 [4, 512, 8, 128], P(('groups', 'outer'), 'inner', 'head'), parts along dimension 0, may hold values from -6 to 6, as said below
- log_total: float32 [4, 8, 512], P(('groups', 'outer'), 'head', 'inner'), parts along dimension 0, as said below
- d_out: bfloat16 [4, 512, 8, 128], P(('groups', 'outer'), 'inner', 'head'), parts along dimension 0, may hold values from -6 to 6
- span_order: int32 [4, 8], P(('groups', 'outer')), parts along dimension 0, may hold values from 0 to 7, as said below
Outputs:
- grad_queries: bfloat16 [4, 512, 8, 128], P(('groups', 'outer'), 'inner', 'head'), parts along dimension 0
- grad_keys: bfloat16 [4, 512, 128], P(('groups', 'outer'), 'inner'), parts along dimension 0
- grad_values: bfloat16 [4, 512, 128], P(('groups', 'outer'), 'inner'), parts along dimension 0
The draws below stay inside these ranges and needn't reach their ends.
There are 2 independent parts, one for each index of `groups`. The reference program is written for one: setup_inputs(seed, part) draws one part's arguments, and reference() takes and returns one part's arrays. A program takes and returns all parts, laid end to end along the dimension named above; each array names one. Nothing has to cross between parts.
Inputs may be any that keep to these rules, and one draw needn't show every extreme that they name: `span_order`: each row is a permutation of 0 to 7. `out`: the causal softmax attention output of queries, keys and values in the order given by span_order, rounded to bfloat16. `log_total`: the log of the causal softmax total of each query row and head for the same inputs.
All inputs are finite; a program needn't handle non-finite values.
Results may differ from the reference program's by a relative error of at most 0.0054.
Values may be sent and summed in bfloat16 or wider, within the bound.
A program may use at most 64 MiB of HBM per device.

```python
import math
import jax
import jax.numpy as jnp
from jax import lax

HD = 128
GROUP_HEADS = 8
SPAN = 64
SEQ = 512
SPANS = 8
BATCH = 2


def layout_positions_drawn(block_order):
    rows = jnp.arange(SEQ, dtype=jnp.int32)
    tok_rows = 2 * SPAN
    owner = rows // tok_rows
    offset = rows % tok_rows
    span = block_order[(2 * owner + offset // SPAN).astype(jnp.int32)]
    return (span * SPAN + offset % SPAN).astype(jnp.int32)


def order_row(row_key):
    return jax.random.permutation(row_key, SPANS)


def base_draw(key):
    order_keys = jax.random.split(jax.random.fold_in(key, 100), BATCH)
    block_order = jax.vmap(order_row)(order_keys).astype(jnp.int32)
    base_keys = jnp.clip(jax.random.normal(jax.random.fold_in(key, 101), (BATCH, SEQ, HD), jnp.float32), -4.0, 4.0)
    base_queries = jnp.clip(jax.random.normal(jax.random.fold_in(key, 102), (BATCH, SEQ, GROUP_HEADS, HD), jnp.float32), -4.0, 4.0)
    base_values = jnp.clip(jax.random.normal(jax.random.fold_in(key, 106), (BATCH, SEQ, HD), jnp.float32), -6.0, 6.0)
    return (base_queries.astype(jnp.bfloat16), base_keys.astype(jnp.bfloat16), base_values.astype(jnp.bfloat16), block_order)


def forward_draw(key):
    queries, keys, values, block_order = base_draw(key)
    softmax_scale = 1.0 / math.sqrt(HD)
    tok_rows = 2 * SPAN

    def one_sequence(items):
        seq_queries, seq_keys, seq_values, seq_order = items
        positions = layout_positions_drawn(seq_order)
        key_float = seq_keys.astype(jnp.float32)
        value_float = seq_values.astype(jnp.float32)

        def one_block(block_index):
            start = (block_index * tok_rows).astype(jnp.int32)
            query_block = lax.dynamic_slice_in_dim(seq_queries, start, tok_rows, 0).astype(jnp.float32)
            query_pos = lax.dynamic_slice_in_dim(positions, start, tok_rows, 0)
            visible = positions[None, :] <= query_pos[:, None]
            scores = jnp.einsum('thd,ud->htu', query_block, key_float) * softmax_scale
            scores = jnp.where(visible[None], scores, -jnp.inf)
            row_max = jnp.max(scores, axis=-1, keepdims=True)
            block_total = row_max + jnp.log(jnp.sum(jnp.exp(scores - row_max), axis=-1, keepdims=True))
            probs = jnp.exp(scores - block_total)
            block_out = jnp.einsum('htu,ud->thd', probs, value_float)
            return (block_out, block_total[:, :, 0])
        outs, totals = lax.map(one_block, jnp.arange(SEQ // tok_rows, dtype=jnp.int32))
        seq_out = outs.reshape(SEQ, GROUP_HEADS, HD).astype(jnp.bfloat16)
        seq_total = jnp.transpose(totals, (1, 0, 2)).reshape(GROUP_HEADS, SEQ)
        return (seq_out, seq_total)
    return lax.map(one_sequence, (queries, keys, values, block_order))


def draw_queries(key, part):
    return base_draw(key)[0]


def draw_keys(key, part):
    return base_draw(key)[1]


def draw_values(key, part):
    return base_draw(key)[2]


def draw_span_order(key, part):
    return base_draw(key)[3]


def draw_out(key, part):
    return forward_draw(key)[0]


def draw_log_total(key, part):
    return forward_draw(key)[1].astype(jnp.float32)


def block_levels(rng, dims, shards, least, largest):
    factor_of = 1.0
    for position, blocks in shards:
        draws = jax.random.uniform(jax.random.fold_in(jax.random.fold_in(rng, 6), position), (blocks,), jnp.float32, least / len(shards), largest / len(shards))
        factor_of = factor_of * jnp.repeat(jnp.exp(draws), dims[position] // blocks).reshape((-1,) + (1,) * (len(dims) - 1 - position))
    return factor_of


def noise(rng, extent, deviation, reach, shards=(), kind=jnp.bfloat16):
    gain = block_levels(rng, extent, shards, -0.22, 0.18) if shards else 1.0
    values = jax.random.normal(rng, extent, jnp.float32) * deviation * gain
    return jnp.minimum(jnp.maximum(values, -reach), reach).astype(kind)


def setup_inputs(seed: int = 0, part: int = 0) -> dict:
    splits = jax.random.split(jax.random.key(seed), 8)
    part_splits = jax.random.split(jax.random.fold_in(splits[7], part), 8)
    return {
        "queries": draw_queries(jax.random.fold_in(jax.random.fold_in(splits[7], part), 71), part),
        "keys": draw_keys(jax.random.fold_in(jax.random.fold_in(splits[7], part), 71), part),
        "values": draw_values(jax.random.fold_in(jax.random.fold_in(splits[7], part), 71), part),
        "out": draw_out(jax.random.fold_in(jax.random.fold_in(splits[7], part), 71), part),
        "log_total": draw_log_total(jax.random.fold_in(jax.random.fold_in(splits[7], part), 71), part),
        "d_out": noise(part_splits[5], (BATCH, SEQ, GROUP_HEADS, HD), 1.0, 6.0, ((0, 2), (1, 4), (2, 2))),
        "span_order": draw_span_order(jax.random.fold_in(jax.random.fold_in(splits[7], part), 71), part),
    }


def layout_positions(block_order):
    rows = jnp.arange(SEQ, dtype=jnp.int32)
    tok_rows = 2 * SPAN
    owner = rows // tok_rows
    offset = rows % tok_rows
    span = block_order[(2 * owner + offset // SPAN).astype(jnp.int32)]
    return (span * SPAN + offset % SPAN).astype(jnp.int32)

def reference(queries, keys, values, out, log_total, d_out, span_order):
    softmax_scale = 1.0 / math.sqrt(HD)
    tok_rows = 2 * SPAN

    def one_sequence(items):
        seq_queries, seq_keys, seq_values, seq_out, seq_total, seq_grad, seq_order = items
        positions = layout_positions(seq_order)
        key_float = seq_keys.astype(jnp.float32)
        value_float = seq_values.astype(jnp.float32)

        def block(carry, block_index):
            key_total, value_total = carry
            start = (block_index * tok_rows).astype(jnp.int32)
            query_block = lax.dynamic_slice_in_dim(seq_queries, start, tok_rows, 0).astype(jnp.float32)
            grad_block = lax.dynamic_slice_in_dim(seq_grad, start, tok_rows, 0).astype(jnp.float32)
            out_block = lax.dynamic_slice_in_dim(seq_out, start, tok_rows, 0).astype(jnp.float32)
            total_block = lax.dynamic_slice_in_dim(seq_total, start, tok_rows, 1)
            query_pos = lax.dynamic_slice_in_dim(positions, start, tok_rows, 0)
            visible = positions[None, :] <= query_pos[:, None]
            scores = jnp.einsum('thd,ud->htu', query_block, key_float) * softmax_scale
            probs = jnp.exp(jnp.where(visible[None], scores - total_block[:, :, None], -jnp.inf))
            grad_probs = jnp.einsum('thd,ud->htu', grad_block, value_float)
            row_delta = jnp.transpose(lax.optimization_barrier(jnp.sum(out_block * grad_block, axis=-1)))[:, :, None]
            grad_scores = probs * (grad_probs - row_delta) * softmax_scale
            scores_half = lax.optimization_barrier(grad_scores.astype(jnp.bfloat16)).astype(jnp.float32)
            probs_half = lax.optimization_barrier(probs.astype(jnp.bfloat16)).astype(jnp.float32)
            query_grad = jnp.einsum('htu,ud->thd', scores_half, key_float).astype(jnp.bfloat16)
            key_total = key_total + jnp.einsum('htu,thd->ud', scores_half, query_block)
            value_total = value_total + jnp.einsum('htu,thd->ud', probs_half, grad_block)
            return ((key_total, value_total), query_grad)
        zeros = jnp.zeros((SEQ, HD), jnp.float32)
        (key_total, value_total), query_grads = lax.scan(block, (zeros, zeros), jnp.arange(SEQ // tok_rows, dtype=jnp.int32))
        grad_queries = query_grads.reshape(SEQ, GROUP_HEADS, HD)
        return (grad_queries, key_total.astype(jnp.bfloat16), value_total.astype(jnp.bfloat16))
    return lax.map(one_sequence, (queries, keys, values, out, log_total, d_out, span_order))
```

```python
import functools
import math

import jax
import jax.numpy as jnp
from jax import lax
from jax.experimental import pallas as pl
from jax.experimental.pallas import tpu as pltpu
from jax.sharding import PartitionSpec as P

MESH = pl.DeviceIdType.MESH
F32 = jnp.float32
BF16 = jnp.bfloat16
NT = (((1,), (1,)), ((), ()))
TN = (((0,), (0,)), ((), ()))
LOG2E = math.log2(math.e)


def dot(a, b, dims=(((1,), (0,)), ((), ()))):
    return lax.dot_general(a, b, dims, preferred_element_type=F32)


def kernel(
    n,
    heads,
    q_hbm,
    k_hbm,
    v_hbm,
    o_hbm,
    l_hbm,
    g_hbm,
    order,
    dq_hbm,
    dk_hbm,
    dv_hbm,
    qs,
    gs,
    os_,
    ls,
    kv,
    stat,
    ds_all,
    part,
    send_buf,
    recv_buf,
    dq_send,
    dq_recv,
    dq_out,
    fin,
    load_sem,
    pair_send,
    pair_recv,
    kv_send,
    kv_recv,
    grad_send,
    grad_recv,
    out_sem,
):
    me = lax.axis_index("inner")
    core = lax.axis_index("head")
    other = 1 - core
    half, width = kv.shape[2], kv.shape[3]
    rows = qs.shape[1]
    scale = 1.0 / math.sqrt(width)
    partner = {"head": other}

    def at(d):
        return {"inner": lax.rem(me + d, n)}

    barrier = pltpu.get_barrier_semaphore()
    for d in range(1, n):
        pl.semaphore_signal(barrier, inc=1, device_id=at(d), device_id_type=MESH)
    pl.semaphore_signal(barrier, inc=1, device_id=partner, device_id_type=MESH)

    mine = pl.ds(pl.multiple_of(core * half, half), half)
    theirs = pl.ds(pl.multiple_of(other * half, half), half)
    loads = [
        pltpu.make_async_copy(src, dst, load_sem.at[i])
        for i, (src, dst) in enumerate(
            (
                (k_hbm.at[mine], kv.at[0, 0]),
                (v_hbm.at[mine], kv.at[0, 1]),
                (q_hbm, qs.at[0]),
                (g_hbm, gs.at[0]),
                (o_hbm, os_.at[0]),
                (l_hbm, ls.at[0]),
            )
        )
    ]
    for load in loads:
        load.start()

    loads[0].wait()
    loads[1].wait()
    pl.semaphore_wait(barrier, n)
    near = sorted(range(1, n), key=lambda d: (-min(d, n - d), d))
    kv_copies = {}
    for d in near:
        kv_copies[d] = pltpu.make_async_remote_copy(
            src_ref=kv.at[0],
            dst_ref=kv.at[d],
            send_sem=kv_send.at[d],
            recv_sem=kv_recv.at[d],
            device_id=at(d),
            device_id_type=MESH,
        )
        kv_copies[d].start()
    pair_copies = []
    for i, ref in enumerate((qs, gs, os_, ls)):
        loads[2 + i].wait()
        copy = pltpu.make_async_remote_copy(
            src_ref=ref.at[0],
            dst_ref=ref.at[1],
            send_sem=pair_send.at[i],
            recv_sem=pair_recv.at[i],
            device_id=partner,
            device_id_type=MESH,
        )
        copy.start()
        pair_copies.append(copy)

    toks = rows // heads
    col = lax.broadcasted_iota(jnp.int32, (toks, rows), 1)
    spread = jnp.where(
        col // heads == lax.broadcasted_iota(jnp.int32, (toks, rows), 0), 1.0, 0.0
    )
    head_of = lax.broadcasted_iota(jnp.int32, (heads, rows), 1) % heads
    pick = head_of == lax.broadcasted_iota(jnp.int32, (heads, rows), 0)
    ones = jnp.ones((8, width), BF16)

    def stats(i):
        total = jnp.dot(
            ls[i], spread, preferred_element_type=F32, precision=lax.Precision.HIGHEST
        )
        total = jnp.sum(jnp.where(pick, total, 0.0), axis=0, keepdims=True)
        prod = os_[i].astype(F32) * gs[i].astype(F32)
        high = prod.astype(BF16)
        low = (prod - high.astype(F32)).astype(BF16)
        delta = dot(ones, high, NT) + dot(ones, low, NT)
        stat[0:1, i * rows : (i + 1) * rows] = total * LOG2E
        stat[1:2, i * rows : (i + 1) * rows] = delta[0:1]

    stats(0)
    for copy in pair_copies:
        copy.wait_recv()
    stats(1)

    tok = (lax.broadcasted_iota(jnp.int32, (1, rows), 1)) // heads
    span = jnp.where(tok < half, order[2 * me], order[2 * me + 1])
    q_pos = span * half + tok % half
    q_pos = jnp.concatenate([q_pos, q_pos], axis=1)
    key_row = lax.broadcasted_iota(jnp.int32, (half, 1), 0)

    def block(d):
        owner = lax.rem(me + (n - d), n)
        k_pos = order[2 * owner + core] * half + key_row
        visible = k_pos <= q_pos
        queries = qs[...].reshape(2 * rows, width)
        grads = gs[...].reshape(2 * rows, width)
        scores = dot(kv[d, 0], queries, NT)
        grad_probs = dot(kv[d, 1], grads, NT)
        probs = jnp.exp2(
            jnp.where(visible, scores * (scale * LOG2E) - stat[0:1, :], -jnp.inf)
        )
        grad_scores = (probs * (grad_probs - stat[1:2, :]) * scale).astype(BF16)
        ds_all[d] = grad_scores
        return dot(grad_scores, queries), dot(probs.astype(BF16), grads)

    part[0], part[1] = block(0)
    grad_copies = {}
    for d in reversed(near):
        kv_copies[d].wait_recv()
        key_grad, value_grad = block(d)
        send_buf[d, 0] = key_grad.astype(BF16)
        send_buf[d, 1] = value_grad.astype(BF16)
        grad_copies[d] = pltpu.make_async_remote_copy(
            src_ref=send_buf.at[d],
            dst_ref=recv_buf.at[d],
            send_sem=grad_send.at[d],
            recv_sem=grad_recv.at[d],
            device_id=at(n - d),
            device_id_type=MESH,
        )
        grad_copies[d].start()

    def query_grad(i):
        total = None
        for d in range(n):
            term = dot(ds_all[d, :, i * rows : (i + 1) * rows], kv[d, 0], TN)
            total = term if total is None else total + term
        return total

    dq_send[...] = query_grad(1)
    dq_copy = pltpu.make_async_remote_copy(
        src_ref=dq_send,
        dst_ref=dq_recv,
        send_sem=pair_send.at[4],
        recv_sem=pair_recv.at[4],
        device_id=partner,
        device_id_type=MESH,
    )
    dq_copy.start()
    own_grad = query_grad(0)
    dq_copy.wait_recv()
    dq_out[...] = (own_grad + dq_recv[...]).astype(BF16)
    outs = [pltpu.make_async_copy(dq_out, dq_hbm, out_sem.at[0])]
    outs[0].start()

    total = part[...]
    for d in reversed(near):
        grad_copies[d].wait_recv()
        total = total + recv_buf[d].astype(F32)
    fin[0] = total.astype(BF16)
    fin_copy = pltpu.make_async_remote_copy(
        src_ref=fin.at[0],
        dst_ref=fin.at[1],
        send_sem=pair_send.at[5],
        recv_sem=pair_recv.at[5],
        device_id=partner,
        device_id_type=MESH,
    )
    fin_copy.start()
    for i, ref in enumerate((dk_hbm, dv_hbm)):
        outs.append(pltpu.make_async_copy(fin.at[0, i], ref.at[mine], out_sem.at[1 + i]))
        outs[-1].start()
    fin_copy.wait_recv()
    for i, ref in enumerate((dk_hbm, dv_hbm)):
        outs.append(pltpu.make_async_copy(fin.at[1, i], ref.at[theirs], out_sem.at[3 + i]))
        outs[-1].start()
    for d in near:
        kv_copies[d].wait_send()
        grad_copies[d].wait_send()
    for copy in pair_copies + [dq_copy, fin_copy]:
        copy.wait_send()
    for out in outs:
        out.wait()


def body(n, queries, keys, values, out, log_total, d_out, span_order):
    _, toks, heads, width = queries.shape
    rows = toks * heads
    half = toks // 2
    flat = lambda x: x.reshape(rows, width)
    anywhere = pl.BlockSpec(memory_space=pl.ANY)
    dq, dk, dv = pl.pallas_call(
        functools.partial(kernel, n, heads),
        out_shape=(
            jax.ShapeDtypeStruct((rows, width), BF16),
            jax.ShapeDtypeStruct((toks, width), BF16),
            jax.ShapeDtypeStruct((toks, width), BF16),
        ),
        in_specs=[anywhere] * 6 + [pl.BlockSpec(memory_space=pltpu.SMEM)],
        out_specs=(anywhere,) * 3,
        scratch_shapes=[
            pltpu.VMEM((2, rows, width), BF16),
            pltpu.VMEM((2, rows, width), BF16),
            pltpu.VMEM((2, rows, width), BF16),
            pltpu.VMEM((2, heads, toks), F32),
            pltpu.VMEM((n, 2, half, width), BF16),
            pltpu.VMEM((8, 2 * rows), F32),
            pltpu.VMEM((n, half, 2 * rows), BF16),
            pltpu.VMEM((2, half, width), F32),
            pltpu.VMEM((n, 2, half, width), BF16),
            pltpu.VMEM((n, 2, half, width), BF16),
            pltpu.VMEM((rows, width), F32),
            pltpu.VMEM((rows, width), F32),
            pltpu.VMEM((rows, width), BF16),
            pltpu.VMEM((2, 2, half, width), BF16),
            pltpu.SemaphoreType.DMA((6,)),
            pltpu.SemaphoreType.DMA((6,)),
            pltpu.SemaphoreType.DMA((6,)),
            pltpu.SemaphoreType.DMA((n,)),
            pltpu.SemaphoreType.DMA((n,)),
            pltpu.SemaphoreType.DMA((n,)),
            pltpu.SemaphoreType.DMA((n,)),
            pltpu.SemaphoreType.DMA((5,)),
        ],
        compiler_params=pltpu.CompilerParams(collective_id=0, has_side_effects=True),
    )(
        flat(queries),
        keys[0],
        values[0],
        flat(out),
        log_total[0],
        flat(d_out),
        span_order[0],
    )
    return dq.reshape(queries.shape), dk[None], dv[None]


def solution(mesh):
    seq = ("groups", "outer")
    wide = P(seq, "inner", "head", None)
    narrow = P(seq, "inner", None)
    return jax.shard_map(
        functools.partial(body, mesh.shape["inner"]),
        mesh=mesh,
        in_specs=(wide, narrow, narrow, wide, P(seq, "head", "inner"), wide, P(seq, None)),
        out_specs=(wide, narrow, narrow),
        check_vma=False,
    )
```

```python
import functools
import math

import jax
import jax.numpy as jnp
from jax import lax
from jax.experimental import pallas as pl
from jax.experimental.pallas import tpu as pltpu
from jax.sharding import PartitionSpec as P

MESH = pl.DeviceIdType.MESH
F32 = jnp.float32
BF16 = jnp.bfloat16
NT = (((1,), (1,)), ((), ()))
TN = (((0,), (0,)), ((), ()))
LOG2E = math.log2(math.e)


def dot(a, b, dims=(((1,), (0,)), ((), ()))):
    return lax.dot_general(a, b, dims, preferred_element_type=F32)


def kernel(
    n,
    heads,
    q_hbm,
    k_hbm,
    v_hbm,
    o_hbm,
    l_hbm,
    g_hbm,
    order,
    dq_ref,
    kv_ref,
    qs,
    gs,
    os_,
    ls,
    kv,
    stat,
    ds_all,
    part,
    send_buf,
    recv_buf,
    dq_send,
    dq_recv,
    fin,
    load_sem,
    pair_send,
    pair_recv,
    kv_send,
    kv_recv,
    grad_send,
    grad_recv,
):
    me = lax.axis_index("inner")
    core = lax.axis_index("head")
    other = 1 - core
    half, width = kv.shape[2], kv.shape[3]
    rows = qs.shape[1]
    scale = 1.0 / math.sqrt(width)
    partner = {"head": other}

    def at(d):
        return {"inner": lax.rem(me + d, n)}

    barrier = pltpu.get_barrier_semaphore()
    for d in range(1, n):
        pl.semaphore_signal(barrier, inc=1, device_id=at(d), device_id_type=MESH)
    pl.semaphore_signal(barrier, inc=1, device_id=partner, device_id_type=MESH)

    mine = pl.ds(pl.multiple_of(core * half, half), half)
    theirs = pl.ds(pl.multiple_of(other * half, half), half)
    loads = [
        pltpu.make_async_copy(src, dst, load_sem.at[i])
        for i, (src, dst) in enumerate(
            (
                (k_hbm.at[mine], kv.at[0, 0]),
                (v_hbm.at[mine], kv.at[0, 1]),
                (q_hbm, qs.at[0]),
                (g_hbm, gs.at[0]),
                (o_hbm, os_.at[0]),
                (l_hbm, ls.at[0]),
            )
        )
    ]
    for load in loads:
        load.start()

    loads[0].wait()
    loads[1].wait()
    pl.semaphore_wait(barrier, n)
    near = sorted(range(1, n), key=lambda d: (-min(d, n - d), d))
    kv_copies = {}
    for d in near:
        kv_copies[d] = pltpu.make_async_remote_copy(
            src_ref=kv.at[0],
            dst_ref=kv.at[d],
            send_sem=kv_send.at[d],
            recv_sem=kv_recv.at[d],
            device_id=at(d),
            device_id_type=MESH,
        )
        kv_copies[d].start()
    pair_copies = []
    for i, ref in enumerate((qs, gs, os_, ls)):
        loads[2 + i].wait()
        copy = pltpu.make_async_remote_copy(
            src_ref=ref.at[0],
            dst_ref=ref.at[1],
            send_sem=pair_send.at[i],
            recv_sem=pair_recv.at[i],
            device_id=partner,
            device_id_type=MESH,
        )
        copy.start()
        pair_copies.append(copy)

    toks = rows // heads
    col = lax.broadcasted_iota(jnp.int32, (toks, rows), 1)
    spread = jnp.where(
        col // heads == lax.broadcasted_iota(jnp.int32, (toks, rows), 0), 1.0, 0.0
    )
    head_of = lax.broadcasted_iota(jnp.int32, (heads, rows), 1) % heads
    pick = head_of == lax.broadcasted_iota(jnp.int32, (heads, rows), 0)
    ones = jnp.ones((8, width), BF16)

    def stats(i):
        total = jnp.dot(
            ls[i], spread, preferred_element_type=F32, precision=lax.Precision.HIGHEST
        )
        total = jnp.sum(jnp.where(pick, total, 0.0), axis=0, keepdims=True)
        prod = os_[i].astype(F32) * gs[i].astype(F32)
        high = prod.astype(BF16)
        low = (prod - high.astype(F32)).astype(BF16)
        delta = dot(ones, high, NT) + dot(ones, low, NT)
        stat[0:1, i * rows : (i + 1) * rows] = total * LOG2E
        stat[1:2, i * rows : (i + 1) * rows] = delta[0:1]

    stats(0)
    for copy in pair_copies:
        copy.wait_recv()
    stats(1)

    tok = (lax.broadcasted_iota(jnp.int32, (1, rows), 1)) // heads
    span = jnp.where(tok < half, order[2 * me], order[2 * me + 1])
    q_pos = span * half + tok % half
    q_pos = jnp.concatenate([q_pos, q_pos], axis=1)
    key_row = lax.broadcasted_iota(jnp.int32, (half, 1), 0)

    def block(d):
        owner = lax.rem(me + (n - d), n)
        k_pos = order[2 * owner + core] * half + key_row
        visible = k_pos <= q_pos
        queries = qs[...].reshape(2 * rows, width)
        grads = gs[...].reshape(2 * rows, width)
        scores = dot(kv[d, 0], queries, NT)
        grad_probs = dot(kv[d, 1], grads, NT)
        probs = jnp.exp2(
            jnp.where(visible, scores * (scale * LOG2E) - stat[0:1, :], -jnp.inf)
        )
        grad_scores = (probs * (grad_probs - stat[1:2, :]) * scale).astype(BF16)
        ds_all[d] = grad_scores
        return dot(grad_scores, queries), dot(probs.astype(BF16), grads)

    part[0], part[1] = block(0)
    grad_copies = {}
    for d in reversed(near):
        kv_copies[d].wait_recv()
        key_grad, value_grad = block(d)
        send_buf[d, 0] = key_grad.astype(BF16)
        send_buf[d, 1] = value_grad.astype(BF16)
        grad_copies[d] = pltpu.make_async_remote_copy(
            src_ref=send_buf.at[d],
            dst_ref=recv_buf.at[d],
            send_sem=grad_send.at[d],
            recv_sem=grad_recv.at[d],
            device_id=at(n - d),
            device_id_type=MESH,
        )
        grad_copies[d].start()

    def query_grad(i):
        total = None
        for d in range(n):
            term = dot(ds_all[d, :, i * rows : (i + 1) * rows], kv[d, 0], TN)
            total = term if total is None else total + term
        return total

    dq_send[...] = query_grad(1)
    dq_copy = pltpu.make_async_remote_copy(
        src_ref=dq_send,
        dst_ref=dq_recv,
        send_sem=pair_send.at[4],
        recv_sem=pair_recv.at[4],
        device_id=partner,
        device_id_type=MESH,
    )
    dq_copy.start()
    own_grad = query_grad(0)
    dq_copy.wait_recv()
    dq_ref[...] = (own_grad + dq_recv[...]).astype(BF16)

    total = part[...]
    for d in reversed(near):
        grad_copies[d].wait_recv()
        total = total + recv_buf[d].astype(F32)
    fin[0] = total.astype(BF16)
    fin_copy = pltpu.make_async_remote_copy(
        src_ref=fin.at[0],
        dst_ref=fin.at[1],
        send_sem=pair_send.at[5],
        recv_sem=pair_recv.at[5],
        device_id=partner,
        device_id_type=MESH,
    )
    fin_copy.start()
    kv_ref[:, mine] = fin[0]
    fin_copy.wait_recv()
    kv_ref[:, theirs] = fin[1]
    for d in near:
        kv_copies[d].wait_send()
        grad_copies[d].wait_send()
    for copy in pair_copies + [dq_copy, fin_copy]:
        copy.wait_send()


def store_kernel(dq_ref, kv_ref, dq_hbm, dk_hbm, dv_hbm, sem):
    pairs = ((dq_ref, dq_hbm), (kv_ref.at[0], dk_hbm), (kv_ref.at[1], dv_hbm))
    copies = [pltpu.make_async_copy(a, b, sem.at[i]) for i, (a, b) in enumerate(pairs)]
    for copy in copies:
        copy.start()
    for copy in copies:
        copy.wait()


def body(n, queries, keys, values, out, log_total, d_out, span_order):
    _, toks, heads, width = queries.shape
    rows = toks * heads
    half = toks // 2
    flat = lambda x: x.reshape(rows, width)
    anywhere = pl.BlockSpec(memory_space=pltpu.HBM)
    in_vmem = pl.BlockSpec(memory_space=pltpu.VMEM)
    dq, dkv = pl.pallas_call(
        functools.partial(kernel, n, heads),
        out_shape=(
            pltpu.VMEM((rows, width), BF16),
            pltpu.VMEM((2, toks, width), BF16),
        ),
        in_specs=[anywhere] * 6 + [pl.BlockSpec(memory_space=pltpu.SMEM)],
        out_specs=(in_vmem,) * 2,
        scratch_shapes=[
            pltpu.VMEM((2, rows, width), BF16),
            pltpu.VMEM((2, rows, width), BF16),
            pltpu.VMEM((2, rows, width), BF16),
            pltpu.VMEM((2, heads, toks), F32),
            pltpu.VMEM((n, 2, half, width), BF16),
            pltpu.VMEM((8, 2 * rows), F32),
            pltpu.VMEM((n, half, 2 * rows), BF16),
            pltpu.VMEM((2, half, width), F32),
            pltpu.VMEM((n, 2, half, width), BF16),
            pltpu.VMEM((n, 2, half, width), BF16),
            pltpu.VMEM((rows, width), F32),
            pltpu.VMEM((rows, width), F32),
            pltpu.VMEM((2, 2, half, width), BF16),
            pltpu.SemaphoreType.DMA((6,)),
            pltpu.SemaphoreType.DMA((6,)),
            pltpu.SemaphoreType.DMA((6,)),
            pltpu.SemaphoreType.DMA((n,)),
            pltpu.SemaphoreType.DMA((n,)),
            pltpu.SemaphoreType.DMA((n,)),
            pltpu.SemaphoreType.DMA((n,)),
        ],
        compiler_params=pltpu.CompilerParams(
            collective_id=0, has_side_effects=True, vmem_limit_bytes=24 * 2**20
        ),
    )(
        flat(queries),
        keys[0],
        values[0],
        flat(out),
        log_total[0],
        flat(d_out),
        span_order[0],
    )
    dq, dk, dv = pl.pallas_call(
        store_kernel,
        out_shape=(
            jax.ShapeDtypeStruct((rows, width), BF16),
            jax.ShapeDtypeStruct((toks, width), BF16),
            jax.ShapeDtypeStruct((toks, width), BF16),
        ),
        in_specs=[in_vmem] * 2,
        out_specs=(anywhere,) * 3,
        scratch_shapes=[pltpu.SemaphoreType.DMA((3,))],
        compiler_params=pltpu.CompilerParams(vmem_limit_bytes=4 * 2**20),
    )(dq, dkv)
    return dq.reshape(queries.shape), dk[None], dv[None]


def solution(mesh):
    seq = ("groups", "outer")
    wide = P(seq, "inner", "head", None)
    narrow = P(seq, "inner", None)
    return jax.shard_map(
        functools.partial(body, mesh.shape["inner"]),
        mesh=mesh,
        in_specs=(wide, narrow, narrow, wide, P(seq, "head", "inner"), wide, P(seq, None)),
        out_specs=(wide, narrow, narrow),
        check_vma=False,
    )
```

```python
import functools
import math

import jax
import jax.numpy as jnp
from jax import lax
from jax.experimental import pallas as pl
from jax.experimental.pallas import tpu as pltpu
from jax.sharding import PartitionSpec as P

MESH = pl.DeviceIdType.MESH
F32 = jnp.float32
BF16 = jnp.bfloat16
NT = (((1,), (1,)), ((), ()))
TN = (((0,), (0,)), ((), ()))
LOG2E = math.log2(math.e)


def dot(a, b, dims=(((1,), (0,)), ((), ()))):
    return lax.dot_general(a, b, dims, preferred_element_type=F32)


def kernel(
    n,
    heads,
    q_hbm,
    k_hbm,
    v_hbm,
    o_hbm,
    l_hbm,
    g_hbm,
    order,
    dq_ref,
    kv_ref,
    qs,
    gs,
    os_,
    ls,
    kv,
    stat,
    ds_all,
    part,
    send_buf,
    recv_buf,
    dq_send,
    dq_recv,
    fin,
    load_sem,
    pair_send,
    pair_recv,
    kv_send,
    kv_recv,
    grad_send,
    grad_recv,
):
    me = lax.axis_index("inner")
    core = lax.axis_index("head")
    other = 1 - core
    half, width = kv.shape[2], kv.shape[3]
    rows = qs.shape[1]
    scale = 1.0 / math.sqrt(width)
    partner = {"head": other}

    def at(d):
        return {"inner": lax.rem(me + d, n)}

    barrier = pltpu.get_barrier_semaphore()
    for d in range(1, n):
        pl.semaphore_signal(barrier, inc=1, device_id=at(d), device_id_type=MESH)
    pl.semaphore_signal(barrier, inc=1, device_id=partner, device_id_type=MESH)

    mine = pl.ds(pl.multiple_of(core * half, half), half)
    theirs = pl.ds(pl.multiple_of(other * half, half), half)
    loads = [
        pltpu.make_async_copy(src, dst, load_sem.at[i])
        for i, (src, dst) in enumerate(
            (
                (k_hbm.at[mine], kv.at[0, 0]),
                (v_hbm.at[mine], kv.at[0, 1]),
                (q_hbm, qs.at[0]),
                (g_hbm, gs.at[0]),
                (o_hbm, os_.at[0]),
                (l_hbm, ls.at[0]),
            )
        )
    ]
    for load in loads:
        load.start()

    loads[0].wait()
    loads[1].wait()
    pl.semaphore_wait(barrier, n)
    near = sorted(range(1, n), key=lambda d: (-min(d, n - d), d))
    kv_copies = {}
    for d in near:
        kv_copies[d] = pltpu.make_async_remote_copy(
            src_ref=kv.at[0],
            dst_ref=kv.at[d],
            send_sem=kv_send.at[d],
            recv_sem=kv_recv.at[d],
            device_id=at(d),
            device_id_type=MESH,
        )
        kv_copies[d].start()
    pair_copies = []
    for i, ref in enumerate((qs, gs, os_, ls)):
        loads[2 + i].wait()
        copy = pltpu.make_async_remote_copy(
            src_ref=ref.at[0],
            dst_ref=ref.at[1],
            send_sem=pair_send.at[i],
            recv_sem=pair_recv.at[i],
            device_id=partner,
            device_id_type=MESH,
        )
        copy.start()
        pair_copies.append(copy)

    toks = rows // heads
    col = lax.broadcasted_iota(jnp.int32, (toks, rows), 1)
    spread = jnp.where(
        col // heads == lax.broadcasted_iota(jnp.int32, (toks, rows), 0), 1.0, 0.0
    )
    head_of = lax.broadcasted_iota(jnp.int32, (heads, rows), 1) % heads
    pick = head_of == lax.broadcasted_iota(jnp.int32, (heads, rows), 0)
    ones = jnp.ones((8, width), BF16)

    def stats(i):
        total = jnp.dot(
            ls[i], spread, preferred_element_type=F32, precision=lax.Precision.HIGHEST
        )
        total = jnp.sum(jnp.where(pick, total, 0.0), axis=0, keepdims=True)
        prod = os_[i].astype(F32) * gs[i].astype(F32)
        high = prod.astype(BF16)
        low = (prod - high.astype(F32)).astype(BF16)
        delta = dot(ones, high, NT) + dot(ones, low, NT)
        stat[0:1, i * rows : (i + 1) * rows] = total * LOG2E
        stat[1:2, i * rows : (i + 1) * rows] = delta[0:1]

    stats(0)
    for copy in pair_copies:
        copy.wait_recv()
    stats(1)

    tok = (lax.broadcasted_iota(jnp.int32, (1, rows), 1)) // heads
    span = jnp.where(tok < half, order[2 * me], order[2 * me + 1])
    q_pos = span * half + tok % half
    q_pos = jnp.concatenate([q_pos, q_pos], axis=1)
    key_row = lax.broadcasted_iota(jnp.int32, (half, 1), 0)

    def block(d):
        owner = lax.rem(me + (n - d), n)
        k_pos = order[2 * owner + core] * half + key_row
        visible = k_pos <= q_pos
        queries = qs[...].reshape(2 * rows, width)
        grads = gs[...].reshape(2 * rows, width)
        scores = dot(kv[d, 0], queries, NT)
        grad_probs = dot(kv[d, 1], grads, NT)
        probs = jnp.exp2(
            jnp.where(visible, scores * (scale * LOG2E) - stat[0:1, :], -jnp.inf)
        )
        grad_scores = (probs * (grad_probs - stat[1:2, :]) * scale).astype(BF16)
        ds_all[d] = grad_scores
        return dot(grad_scores, queries), dot(probs.astype(BF16), grads)

    part[0], part[1] = block(0)
    grad_copies = {}
    for d in reversed(near):
        kv_copies[d].wait_recv()
        key_grad, value_grad = block(d)
        send_buf[d, 0] = key_grad.astype(BF16)
        send_buf[d, 1] = value_grad.astype(BF16)
        grad_copies[d] = pltpu.make_async_remote_copy(
            src_ref=send_buf.at[d],
            dst_ref=recv_buf.at[d],
            send_sem=grad_send.at[d],
            recv_sem=grad_recv.at[d],
            device_id=at(n - d),
            device_id_type=MESH,
        )
        grad_copies[d].start()

    def query_grad(i):
        total = None
        for d in range(n):
            term = dot(ds_all[d, :, i * rows : (i + 1) * rows], kv[d, 0], TN)
            total = term if total is None else total + term
        return total

    dq_send[...] = query_grad(1)
    dq_copy = pltpu.make_async_remote_copy(
        src_ref=dq_send,
        dst_ref=dq_recv,
        send_sem=pair_send.at[4],
        recv_sem=pair_recv.at[4],
        device_id=partner,
        device_id_type=MESH,
    )
    dq_copy.start()
    own_grad = query_grad(0)
    dq_copy.wait_recv()
    dq_ref[...] = (own_grad + dq_recv[...]).astype(BF16)

    total = part[...]
    for d in reversed(near):
        grad_copies[d].wait_recv()
        total = total + recv_buf[d].astype(F32)
    fin[0] = total.astype(BF16)
    fin_copy = pltpu.make_async_remote_copy(
        src_ref=fin.at[0],
        dst_ref=fin.at[1],
        send_sem=pair_send.at[5],
        recv_sem=pair_recv.at[5],
        device_id=partner,
        device_id_type=MESH,
    )
    fin_copy.start()
    kv_ref[:, mine] = fin[0]
    fin_copy.wait_recv()
    kv_ref[:, theirs] = fin[1]
    for d in near:
        kv_copies[d].wait_send()
        grad_copies[d].wait_send()
    for copy in pair_copies + [dq_copy, fin_copy]:
        copy.wait_send()


def store_kernel(dq_ref, kv_ref, dq_hbm, dk_hbm, dv_hbm, sem):
    pairs = ((dq_ref, dq_hbm), (kv_ref.at[0], dk_hbm), (kv_ref.at[1], dv_hbm))
    copies = [pltpu.make_async_copy(a, b, sem.at[i]) for i, (a, b) in enumerate(pairs)]
    for copy in copies:
        copy.start()
    for copy in copies:
        copy.wait()


def body(n, queries, keys, values, out, log_total, d_out, span_order):
    _, toks, heads, width = queries.shape
    rows = toks * heads
    half = toks // 2
    flat = lambda x: x.reshape(rows, width)
    anywhere = pl.BlockSpec(memory_space=pltpu.HBM)
    in_vmem = pl.BlockSpec(memory_space=pltpu.VMEM)
    dq, dkv = pl.pallas_call(
        functools.partial(kernel, n, heads),
        out_shape=(
            pltpu.VMEM((rows, width), BF16),
            pltpu.VMEM((2, toks, width), BF16),
        ),
        in_specs=[anywhere] * 6 + [pl.BlockSpec(memory_space=pltpu.SMEM)],
        out_specs=(in_vmem,) * 2,
        scratch_shapes=[
            pltpu.VMEM((2, rows, width), BF16),
            pltpu.VMEM((2, rows, width), BF16),
            pltpu.VMEM((2, rows, width), BF16),
            pltpu.VMEM((2, heads, toks), F32),
            pltpu.VMEM((n, 2, half, width), BF16),
            pltpu.VMEM((8, 2 * rows), F32),
            pltpu.VMEM((n, half, 2 * rows), BF16),
            pltpu.VMEM((2, half, width), F32),
            pltpu.VMEM((n, 2, half, width), BF16),
            pltpu.VMEM((n, 2, half, width), BF16),
            pltpu.VMEM((rows, width), F32),
            pltpu.VMEM((rows, width), F32),
            pltpu.VMEM((2, 2, half, width), BF16),
            pltpu.SemaphoreType.DMA((6,)),
            pltpu.SemaphoreType.DMA((6,)),
            pltpu.SemaphoreType.DMA((6,)),
            pltpu.SemaphoreType.DMA((n,)),
            pltpu.SemaphoreType.DMA((n,)),
            pltpu.SemaphoreType.DMA((n,)),
            pltpu.SemaphoreType.DMA((n,)),
        ],
        compiler_params=pltpu.CompilerParams(collective_id=0, has_side_effects=True),
    )(
        flat(queries),
        keys[0],
        values[0],
        flat(out),
        log_total[0],
        flat(d_out),
        span_order[0],
    )
    dq, dk, dv = pl.pallas_call(
        store_kernel,
        out_shape=(
            jax.ShapeDtypeStruct((rows, width), BF16),
            jax.ShapeDtypeStruct((toks, width), BF16),
            jax.ShapeDtypeStruct((toks, width), BF16),
        ),
        in_specs=[in_vmem] * 2,
        out_specs=(anywhere,) * 3,
        scratch_shapes=[pltpu.SemaphoreType.DMA((3,))],
        compiler_params=pltpu.CompilerParams(vmem_limit_bytes=2**20),
    )(dq, dkv)
    return dq.reshape(queries.shape), dk[None], dv[None]


def solution(mesh):
    seq = ("groups", "outer")
    wide = P(seq, "inner", "head", None)
    narrow = P(seq, "inner", None)
    return jax.shard_map(
        functools.partial(body, mesh.shape["inner"]),
        mesh=mesh,
        in_specs=(wide, narrow, narrow, wide, P(seq, "head", "inner"), wide, P(seq, None)),
        out_specs=(wide, narrow, narrow),
        check_vma=False,
    )
```

```python
import functools
import math

import jax
import jax.numpy as jnp
from jax import lax
from jax.experimental import pallas as pl
from jax.experimental.pallas import tpu as pltpu
from jax.sharding import PartitionSpec as P

MESH = pl.DeviceIdType.MESH
F32 = jnp.float32
BF16 = jnp.bfloat16
NT = (((1,), (1,)), ((), ()))
TN = (((0,), (0,)), ((), ()))
LOG2E = math.log2(math.e)


def dot(a, b, dims=(((1,), (0,)), ((), ()))):
    return lax.dot_general(a, b, dims, preferred_element_type=F32)


def kernel(
    n,
    heads,
    q_hbm,
    k_hbm,
    v_hbm,
    o_hbm,
    l_hbm,
    g_hbm,
    order_hbm,
    dq_ref,
    kv_ref,
    qs,
    gs,
    os_,
    ls,
    kv,
    stat,
    ds_all,
    part,
    send_buf,
    recv_buf,
    dq_send,
    dq_recv,
    fin,
    order,
    load_sem,
    pair_send,
    pair_recv,
    kv_send,
    kv_recv,
    grad_send,
    grad_recv,
):
    me = lax.axis_index("inner")
    core = lax.axis_index("head")
    other = 1 - core
    half, width = kv.shape[2], kv.shape[3]
    rows = qs.shape[1]
    scale = 1.0 / math.sqrt(width)
    partner = {"head": other}

    def at(d):
        return {"inner": lax.rem(me + d, n)}

    barrier = pltpu.get_barrier_semaphore()
    for d in range(1, n):
        pl.semaphore_signal(barrier, inc=1, device_id=at(d), device_id_type=MESH)
    pl.semaphore_signal(barrier, inc=1, device_id=partner, device_id_type=MESH)

    mine = pl.ds(pl.multiple_of(core * half, half), half)
    theirs = pl.ds(pl.multiple_of(other * half, half), half)
    loads = [
        pltpu.make_async_copy(src, dst, load_sem.at[i])
        for i, (src, dst) in enumerate(
            (
                (k_hbm.at[mine], kv.at[0, 0]),
                (v_hbm.at[mine], kv.at[0, 1]),
                (q_hbm, qs.at[0]),
                (g_hbm, gs.at[0]),
                (o_hbm, os_.at[0]),
                (l_hbm, ls.at[0]),
                (order_hbm, order),
            )
        )
    ]
    for load in loads:
        load.start()

    loads[0].wait()
    loads[1].wait()
    pl.semaphore_wait(barrier, n)
    near = sorted(range(1, n), key=lambda d: (-min(d, n - d), d))
    kv_copies = {}
    for d in near:
        kv_copies[d] = pltpu.make_async_remote_copy(
            src_ref=kv.at[0],
            dst_ref=kv.at[d],
            send_sem=kv_send.at[d],
            recv_sem=kv_recv.at[d],
            device_id=at(d),
            device_id_type=MESH,
        )
        kv_copies[d].start()
    pair_copies = []
    for i, ref in enumerate((qs, gs, os_, ls)):
        loads[2 + i].wait()
        copy = pltpu.make_async_remote_copy(
            src_ref=ref.at[0],
            dst_ref=ref.at[1],
            send_sem=pair_send.at[i],
            recv_sem=pair_recv.at[i],
            device_id=partner,
            device_id_type=MESH,
        )
        copy.start()
        pair_copies.append(copy)

    toks = rows // heads
    col = lax.broadcasted_iota(jnp.int32, (toks, rows), 1)
    spread = jnp.where(
        col // heads == lax.broadcasted_iota(jnp.int32, (toks, rows), 0), 1.0, 0.0
    )
    head_of = lax.broadcasted_iota(jnp.int32, (heads, rows), 1) % heads
    pick = head_of == lax.broadcasted_iota(jnp.int32, (heads, rows), 0)
    ones = jnp.ones((8, width), BF16)

    def stats(i):
        total = jnp.dot(
            ls[i], spread, preferred_element_type=F32, precision=lax.Precision.HIGHEST
        )
        total = jnp.sum(jnp.where(pick, total, 0.0), axis=0, keepdims=True)
        prod = os_[i].astype(F32) * gs[i].astype(F32)
        high = prod.astype(BF16)
        low = (prod - high.astype(F32)).astype(BF16)
        delta = dot(ones, high, NT) + dot(ones, low, NT)
        stat[0:1, i * rows : (i + 1) * rows] = total * LOG2E
        stat[1:2, i * rows : (i + 1) * rows] = delta[0:1]

    stats(0)
    for copy in pair_copies:
        copy.wait_recv()
    stats(1)

    loads[6].wait()
    tok = (lax.broadcasted_iota(jnp.int32, (1, rows), 1)) // heads
    span = jnp.where(tok < half, order[2 * me], order[2 * me + 1])
    q_pos = span * half + tok % half
    q_pos = jnp.concatenate([q_pos, q_pos], axis=1)
    key_row = lax.broadcasted_iota(jnp.int32, (half, 1), 0)

    def block(d):
        owner = lax.rem(me + (n - d), n)
        k_pos = order[2 * owner + core] * half + key_row
        visible = k_pos <= q_pos
        queries = qs[...].reshape(2 * rows, width)
        grads = gs[...].reshape(2 * rows, width)
        scores = dot(kv[d, 0], queries, NT)
        grad_probs = dot(kv[d, 1], grads, NT)
        probs = jnp.exp2(
            jnp.where(visible, scores * (scale * LOG2E) - stat[0:1, :], -jnp.inf)
        )
        grad_scores = (probs * (grad_probs - stat[1:2, :]) * scale).astype(BF16)
        ds_all[d] = grad_scores
        return dot(grad_scores, queries), dot(probs.astype(BF16), grads)

    part[0], part[1] = block(0)
    grad_copies = {}
    for d in reversed(near):
        kv_copies[d].wait_recv()
        key_grad, value_grad = block(d)
        send_buf[d, 0] = key_grad.astype(BF16)
        send_buf[d, 1] = value_grad.astype(BF16)
        grad_copies[d] = pltpu.make_async_remote_copy(
            src_ref=send_buf.at[d],
            dst_ref=recv_buf.at[d],
            send_sem=grad_send.at[d],
            recv_sem=grad_recv.at[d],
            device_id=at(n - d),
            device_id_type=MESH,
        )
        grad_copies[d].start()

    def query_grad(i):
        total = None
        for d in range(n):
            term = dot(ds_all[d, :, i * rows : (i + 1) * rows], kv[d, 0], TN)
            total = term if total is None else total + term
        return total

    dq_send[...] = query_grad(1)
    dq_copy = pltpu.make_async_remote_copy(
        src_ref=dq_send,
        dst_ref=dq_recv,
        send_sem=pair_send.at[4],
        recv_sem=pair_recv.at[4],
        device_id=partner,
        device_id_type=MESH,
    )
    dq_copy.start()
    own_grad = query_grad(0)
    dq_copy.wait_recv()
    dq_ref[...] = (own_grad + dq_recv[...]).astype(BF16)

    total = part[...]
    for d in reversed(near):
        grad_copies[d].wait_recv()
        total = total + recv_buf[d].astype(F32)
    fin[0] = total.astype(BF16)
    fin_copy = pltpu.make_async_remote_copy(
        src_ref=fin.at[0],
        dst_ref=fin.at[1],
        send_sem=pair_send.at[5],
        recv_sem=pair_recv.at[5],
        device_id=partner,
        device_id_type=MESH,
    )
    fin_copy.start()
    kv_ref[:, mine] = fin[0]
    fin_copy.wait_recv()
    kv_ref[:, theirs] = fin[1]
    for d in near:
        kv_copies[d].wait_send()
        grad_copies[d].wait_send()
    for copy in pair_copies + [dq_copy, fin_copy]:
        copy.wait_send()


def store_kernel(dq_ref, kv_ref, dq_hbm, dk_hbm, dv_hbm, sem):
    pairs = ((dq_ref, dq_hbm), (kv_ref.at[0], dk_hbm), (kv_ref.at[1], dv_hbm))
    copies = [pltpu.make_async_copy(a, b, sem.at[i]) for i, (a, b) in enumerate(pairs)]
    for copy in copies:
        copy.start()
    for copy in copies:
        copy.wait()


def body(n, queries, keys, values, out, log_total, d_out, span_order):
    _, toks, heads, width = queries.shape
    rows = toks * heads
    half = toks // 2
    flat = lambda x: x.reshape(rows, width)
    anywhere = pl.BlockSpec(memory_space=pltpu.HBM)
    in_vmem = pl.BlockSpec(memory_space=pltpu.VMEM)
    dq, dkv = pl.pallas_call(
        functools.partial(kernel, n, heads),
        out_shape=(
            pltpu.VMEM((rows, width), BF16),
            pltpu.VMEM((2, toks, width), BF16),
        ),
        in_specs=[anywhere] * 7,
        out_specs=(in_vmem,) * 2,
        scratch_shapes=[
            pltpu.VMEM((2, rows, width), BF16),
            pltpu.VMEM((2, rows, width), BF16),
            pltpu.VMEM((2, rows, width), BF16),
            pltpu.VMEM((2, heads, toks), F32),
            pltpu.VMEM((n, 2, half, width), BF16),
            pltpu.VMEM((8, 2 * rows), F32),
            pltpu.VMEM((n, half, 2 * rows), BF16),
            pltpu.VMEM((2, half, width), F32),
            pltpu.VMEM((n, 2, half, width), BF16),
            pltpu.VMEM((n, 2, half, width), BF16),
            pltpu.VMEM((rows, width), F32),
            pltpu.VMEM((rows, width), F32),
            pltpu.VMEM((2, 2, half, width), BF16),
            pltpu.SMEM((span_order.shape[1],), jnp.int32),
            pltpu.SemaphoreType.DMA((7,)),
            pltpu.SemaphoreType.DMA((6,)),
            pltpu.SemaphoreType.DMA((6,)),
            pltpu.SemaphoreType.DMA((n,)),
            pltpu.SemaphoreType.DMA((n,)),
            pltpu.SemaphoreType.DMA((n,)),
            pltpu.SemaphoreType.DMA((n,)),
        ],
        compiler_params=pltpu.CompilerParams(collective_id=0, has_side_effects=True),
    )(
        flat(queries),
        keys[0],
        values[0],
        flat(out),
        log_total[0],
        flat(d_out),
        span_order[0],
    )
    dq, dk, dv = pl.pallas_call(
        store_kernel,
        out_shape=(
            jax.ShapeDtypeStruct((rows, width), BF16),
            jax.ShapeDtypeStruct((toks, width), BF16),
            jax.ShapeDtypeStruct((toks, width), BF16),
        ),
        in_specs=[in_vmem] * 2,
        out_specs=(anywhere,) * 3,
        scratch_shapes=[pltpu.SemaphoreType.DMA((3,))],
        compiler_params=pltpu.CompilerParams(vmem_limit_bytes=2**20),
    )(dq, dkv)
    return dq.reshape(queries.shape), dk[None], dv[None]


def solution(mesh):
    seq = ("groups", "outer")
    wide = P(seq, "inner", "head", None)
    narrow = P(seq, "inner", None)
    return jax.shard_map(
        functools.partial(body, mesh.shape["inner"]),
        mesh=mesh,
        in_specs=(wide, narrow, narrow, wide, P(seq, "head", "inner"), wide, P(seq, None)),
        out_specs=(wide, narrow, narrow),
        check_vma=False,
    )
```

```python
import functools
import math

import jax
import jax.numpy as jnp
from jax import lax
from jax.experimental import pallas as pl
from jax.experimental.pallas import tpu as pltpu
from jax.sharding import PartitionSpec as P

MESH = pl.DeviceIdType.MESH
F32 = jnp.float32
BF16 = jnp.bfloat16
NT = (((1,), (1,)), ((), ()))
TN = (((0,), (0,)), ((), ()))
LOG2E = math.log2(math.e)


def dot(a, b, dims=(((1,), (0,)), ((), ()))):
    return lax.dot_general(a, b, dims, preferred_element_type=F32)


def kernel(
    n,
    heads,
    q_hbm,
    k_hbm,
    v_hbm,
    o_hbm,
    l_hbm,
    g_hbm,
    order_hbm,
    dq_ref,
    kv_ref,
    qs,
    gs,
    os_,
    ls,
    kv,
    stat,
    ds_all,
    part,
    send_buf,
    recv_buf,
    dq_send,
    dq_recv,
    fin,
    order,
    load_sem,
    pair_send,
    pair_recv,
    kv_send,
    kv_recv,
    grad_send,
    grad_recv,
):
    me = lax.axis_index("inner")
    core = lax.axis_index("head")
    other = 1 - core
    half, width = kv.shape[2], kv.shape[3]
    rows = qs.shape[1]
    scale = 1.0 / math.sqrt(width)
    partner = {"head": other}

    def at(d):
        return {"inner": lax.rem(me + d, n)}

    barrier = pltpu.get_barrier_semaphore()
    near = sorted(range(1, n), key=lambda d: (-min(d, n - d), d))
    for d in near:
        pl.semaphore_signal(barrier, inc=1, device_id=at(d), device_id_type=MESH)
    pl.semaphore_signal(barrier, inc=1, device_id=partner, device_id_type=MESH)

    mine = pl.ds(pl.multiple_of(core * half, half), half)
    theirs = pl.ds(pl.multiple_of(other * half, half), half)
    loads = [
        pltpu.make_async_copy(src, dst, load_sem.at[i])
        for i, (src, dst) in enumerate(
            (
                (k_hbm.at[mine], kv.at[0, 0]),
                (v_hbm.at[mine], kv.at[0, 1]),
                (q_hbm, qs.at[0]),
                (g_hbm, gs.at[0]),
                (o_hbm, os_.at[0]),
                (l_hbm, ls.at[0]),
                (order_hbm, order),
            )
        )
    ]
    for load in loads:
        load.start()

    loads[0].wait()
    loads[1].wait()
    pl.semaphore_wait(barrier, n)
    kv_copies = {}
    for d in near:
        kv_copies[d] = pltpu.make_async_remote_copy(
            src_ref=kv.at[0],
            dst_ref=kv.at[d],
            send_sem=kv_send.at[d],
            recv_sem=kv_recv.at[d],
            device_id=at(d),
            device_id_type=MESH,
        )
        kv_copies[d].start()
    pair_copies = []
    for i, ref in enumerate((qs, gs, os_, ls)):
        loads[2 + i].wait()
        copy = pltpu.make_async_remote_copy(
            src_ref=ref.at[0],
            dst_ref=ref.at[1],
            send_sem=pair_send.at[i],
            recv_sem=pair_recv.at[i],
            device_id=partner,
            device_id_type=MESH,
        )
        copy.start()
        pair_copies.append(copy)

    toks = rows // heads
    col = lax.broadcasted_iota(jnp.int32, (toks, rows), 1)
    spread = jnp.where(
        col // heads == lax.broadcasted_iota(jnp.int32, (toks, rows), 0), 1.0, 0.0
    )
    head_of = lax.broadcasted_iota(jnp.int32, (heads, rows), 1) % heads
    pick = head_of == lax.broadcasted_iota(jnp.int32, (heads, rows), 0)
    ones = jnp.ones((8, width), BF16)

    def stats(i):
        total = jnp.dot(
            ls[i], spread, preferred_element_type=F32, precision=lax.Precision.HIGHEST
        )
        total = jnp.sum(jnp.where(pick, total, 0.0), axis=0, keepdims=True)
        prod = os_[i].astype(F32) * gs[i].astype(F32)
        high = prod.astype(BF16)
        low = (prod - high.astype(F32)).astype(BF16)
        delta = dot(ones, high, NT) + dot(ones, low, NT)
        stat[0:1, i * rows : (i + 1) * rows] = total * LOG2E
        stat[1:2, i * rows : (i + 1) * rows] = delta[0:1]

    stats(0)
    for copy in pair_copies:
        copy.wait_recv()
    stats(1)

    loads[6].wait()
    tok = (lax.broadcasted_iota(jnp.int32, (1, rows), 1)) // heads
    span = jnp.where(tok < half, order[2 * me], order[2 * me + 1])
    q_pos = span * half + tok % half
    q_pos = jnp.concatenate([q_pos, q_pos], axis=1)
    key_row = lax.broadcasted_iota(jnp.int32, (half, 1), 0)

    def block(d):
        owner = lax.rem(me + (n - d), n)
        k_pos = order[2 * owner + core] * half + key_row
        visible = k_pos <= q_pos
        queries = qs[...].reshape(2 * rows, width)
        grads = gs[...].reshape(2 * rows, width)
        scores = dot(kv[d, 0], queries, NT)
        grad_probs = dot(kv[d, 1], grads, NT)
        probs = jnp.exp2(
            jnp.where(visible, scores * (scale * LOG2E) - stat[0:1, :], -jnp.inf)
        )
        grad_scores = (probs * (grad_probs - stat[1:2, :]) * scale).astype(BF16)
        ds_all[d] = grad_scores
        yield 1, dot(probs.astype(BF16), grads)
        yield 0, dot(grad_scores, queries)

    for i, grad in block(0):
        part[i] = grad
    grad_copies = {}
    for d in reversed(near):
        kv_copies[d].wait_recv()
        for i, grad in block(d):
            send_buf[d, i] = grad.astype(BF16)
            grad_copies[d, i] = pltpu.make_async_remote_copy(
                src_ref=send_buf.at[d, i],
                dst_ref=recv_buf.at[d, i],
                send_sem=grad_send.at[d, i],
                recv_sem=grad_recv.at[d, i],
                device_id=at(n - d),
                device_id_type=MESH,
            )
            grad_copies[d, i].start()

    def query_grad(i):
        total = None
        for d in range(n):
            term = dot(ds_all[d, :, i * rows : (i + 1) * rows], kv[d, 0], TN)
            total = term if total is None else total + term
        return total

    dq_send[...] = query_grad(1)
    dq_copy = pltpu.make_async_remote_copy(
        src_ref=dq_send,
        dst_ref=dq_recv,
        send_sem=pair_send.at[4],
        recv_sem=pair_recv.at[4],
        device_id=partner,
        device_id_type=MESH,
    )
    dq_copy.start()
    own_grad = query_grad(0)
    dq_copy.wait_recv()
    dq_ref[...] = (own_grad + dq_recv[...]).astype(BF16)

    fin_copies = []
    for i in (1, 0):
        total = part[i]
        for d in reversed(near):
            grad_copies[d, i].wait_recv()
            total = total + recv_buf[d, i].astype(F32)
        fin[0, i] = total.astype(BF16)
        copy = pltpu.make_async_remote_copy(
            src_ref=fin.at[0, i],
            dst_ref=fin.at[1, i],
            send_sem=pair_send.at[5 + i],
            recv_sem=pair_recv.at[5 + i],
            device_id=partner,
            device_id_type=MESH,
        )
        copy.start()
        fin_copies.append(copy)
    kv_ref[:, mine] = fin[0]
    for copy in fin_copies:
        copy.wait_recv()
    kv_ref[:, theirs] = fin[1]
    for d in near:
        kv_copies[d].wait_send()
        grad_copies[d, 0].wait_send()
        grad_copies[d, 1].wait_send()
    for copy in pair_copies + [dq_copy] + fin_copies:
        copy.wait_send()


def store_kernel(dq_ref, kv_ref, dq_hbm, dk_hbm, dv_hbm, sem):
    pairs = ((dq_ref, dq_hbm), (kv_ref.at[0], dk_hbm), (kv_ref.at[1], dv_hbm))
    copies = [pltpu.make_async_copy(a, b, sem.at[i]) for i, (a, b) in enumerate(pairs)]
    for copy in copies:
        copy.start()
    for copy in copies:
        copy.wait()


def body(n, queries, keys, values, out, log_total, d_out, span_order):
    _, toks, heads, width = queries.shape
    rows = toks * heads
    half = toks // 2
    flat = lambda x: x.reshape(rows, width)
    anywhere = pl.BlockSpec(memory_space=pltpu.HBM)
    in_vmem = pl.BlockSpec(memory_space=pltpu.VMEM)
    dq, dkv = pl.pallas_call(
        functools.partial(kernel, n, heads),
        out_shape=(
            pltpu.VMEM((rows, width), BF16),
            pltpu.VMEM((2, toks, width), BF16),
        ),
        in_specs=[anywhere] * 7,
        out_specs=(in_vmem,) * 2,
        scratch_shapes=[
            pltpu.VMEM((2, rows, width), BF16),
            pltpu.VMEM((2, rows, width), BF16),
            pltpu.VMEM((2, rows, width), BF16),
            pltpu.VMEM((2, heads, toks), F32),
            pltpu.VMEM((n, 2, half, width), BF16),
            pltpu.VMEM((8, 2 * rows), F32),
            pltpu.VMEM((n, half, 2 * rows), BF16),
            pltpu.VMEM((2, half, width), F32),
            pltpu.VMEM((n, 2, half, width), BF16),
            pltpu.VMEM((n, 2, half, width), BF16),
            pltpu.VMEM((rows, width), F32),
            pltpu.VMEM((rows, width), F32),
            pltpu.VMEM((2, 2, half, width), BF16),
            pltpu.SMEM((span_order.shape[1],), jnp.int32),
            pltpu.SemaphoreType.DMA((7,)),
            pltpu.SemaphoreType.DMA((7,)),
            pltpu.SemaphoreType.DMA((7,)),
            pltpu.SemaphoreType.DMA((n,)),
            pltpu.SemaphoreType.DMA((n,)),
            pltpu.SemaphoreType.DMA((n, 2)),
            pltpu.SemaphoreType.DMA((n, 2)),
        ],
        compiler_params=pltpu.CompilerParams(collective_id=0, has_side_effects=True),
    )(
        flat(queries),
        keys[0],
        values[0],
        flat(out),
        log_total[0],
        flat(d_out),
        span_order[0],
    )
    dq, dk, dv = pl.pallas_call(
        store_kernel,
        out_shape=(
            jax.ShapeDtypeStruct((rows, width), BF16),
            jax.ShapeDtypeStruct((toks, width), BF16),
            jax.ShapeDtypeStruct((toks, width), BF16),
        ),
        in_specs=[in_vmem] * 2,
        out_specs=(anywhere,) * 3,
        scratch_shapes=[pltpu.SemaphoreType.DMA((3,))],
        compiler_params=pltpu.CompilerParams(vmem_limit_bytes=2**20),
    )(dq, dkv)
    return dq.reshape(queries.shape), dk[None], dv[None]


def solution(mesh):
    seq = ("groups", "outer")
    wide = P(seq, "inner", "head", None)
    narrow = P(seq, "inner", None)
    return jax.shard_map(
        functools.partial(body, mesh.shape["inner"]),
        mesh=mesh,
        in_specs=(wide, narrow, narrow, wide, P(seq, "head", "inner"), wide, P(seq, None)),
        out_specs=(wide, narrow, narrow),
        check_vma=False,
    )
```
